32 devices in a mesh: member: 4 (over y, core), lat: 8 (over z, x).
Axes of the slice: x: 2, y: 2, z: 4, core: 2. Of those that a mesh axis runs over, the one named last changes fastest.
Arguments:
- ensemble: float32 [640, 32, 256], P('member', 'lat'), may hold values from -6 to 6
- obs_cell: int32 [32, 128], P(('member', 'lat')), may hold values from 0 to 255
- obs_value: float32 [32, 128], P(('member', 'lat')), may hold values from -8 to 8
- obs_var: float32 [32, 128], P(('member', 'lat')), may hold values from 0.5 to 8
- patch_rows: int32 [32, 2], P(('member', 'lat')), may hold values from 1 to 24, 32 in all within a row
Outputs:
- analysis: float32 [640, 32, 256], P('member', 'lat')
The draws below stay inside these ranges and needn't reach their ends.
Inputs may be any that keep to these rules, and one draw needn't show every extreme that they name: `patch_rows`: each server's 2 patch lengths sum to 32.
All inputs are finite; a program needn't handle non-finite values. Where the reference program divides by a largest or mean magnitude, that divisor is 1e-20 or more.
Results may differ from the reference program's by a relative error of at most 0.0003.
Values sent between devices are 32-bit elements; how exact they have to be, the bound alone decides.
A program may use at most 64 MiB of HBM per device.

```python
import math
import jax
import jax.numpy as jnp
import numpy as np
from jax import lax

K = 640
LON_DEV = 8
OBS_DEV = 128
PATCH_DEV = 2
NS_ITERS = 3
STEPS = 4
NLAT = 32
NLON = 256
DEVICES = 32


def place_ends(drawn, own_key, low, top_value):
    longest = drawn.shape.index(max(drawn.shape))
    spots = []
    for shift in (0, 1):
        where = [jax.random.randint(jax.random.fold_in(own_key, axis), (), 0, length) for axis, length in enumerate(drawn.shape)]
        where[longest] = (where[longest] + shift) % drawn.shape[longest]
        spots.append(tuple(where))
    return drawn.at[spots[0]].set(low).at[spots[1]].set(top_value)


def steps_of(key, extent, shards, smallest, largest):
    level = 1.0
    for position, blocks in shards:
        draws = jax.random.uniform(jax.random.fold_in(jax.random.fold_in(key, 6), position), (blocks,), jnp.float32, smallest / len(shards), largest / len(shards))
        level = level * jnp.repeat(jnp.exp(draws), extent[position] // blocks).reshape((-1,) + (1,) * (len(extent) - 1 - position))
    return level


def profile(count, total, most, skew):
    portions = [(1 << 20) // math.isqrt(grade ** skew) + 1 for grade in range(2, count + 1)]
    rest, counts = total - most - (count - 1), [1] * (count - 1)
    while rest > 0:
        free = [i for i in range(count - 1) if counts[i] < most]
        pool, budget = sum([portions[i] for i in free]), rest
        for i in free:
            more = min(most - counts[i], max(1, budget * portions[i] // pool), rest)
            counts[i] = counts[i] + more
            rest = rest - more
    return np.array([most] + counts)


def ragged_sizes(own_key, amount, total, limit, skew):
    if amount == 2:
        one = jax.random.randint(own_key, (), max(1, total - limit), min(limit, total - 1) + 1)
        return jnp.stack([one, total - one])
    sizes = jnp.asarray(profile(amount, total, limit, skew), jnp.int32)
    twos = (amount - 1) // 2
    source_of, taker = sizes[1:1 + 2 * twos:2], sizes[2:2 + 2 * twos:2]
    slack = jnp.minimum(source_of - 1, limit - taker)
    shifted = jax.random.randint(jax.random.fold_in(own_key, 1), (twos,), 0, 1 << 20) % (slack + 1)
    sizes = sizes.at[1:1 + 2 * twos:2].set(source_of - shifted).at[2:2 + 2 * twos:2].set(taker + shifted)
    return sizes[jax.random.permutation(jax.random.fold_in(own_key, 2), amount)]


def gaussian(rng, shape, scale, limit, cuts=(), kind=jnp.bfloat16):
    values = jax.random.normal(rng, shape, jnp.float32) * scale
    if len(cuts) > 0:
        values = steps_of(rng, shape, cuts, -0.22, 0.18) * values
    return jnp.clip(values, min=-limit, max=limit).astype(kind)


def setup_inputs(seed: int = 0) -> dict:
    key_list = jax.random.split(jax.random.key(seed), 6)
    return {
        "ensemble": gaussian(key_list[0], (K, NLAT, NLON), 1.0, 6.0, ((0, 4), (1, 8)), jnp.float32),
        "obs_cell": place_ends(jax.random.randint(key_list[1], (DEVICES, OBS_DEV), 0, NLAT * LON_DEV), jax.random.fold_in(key_list[1], 1), 0, (NLAT * LON_DEV) - 1).astype(jnp.int32),
        "obs_value": gaussian(key_list[2], (DEVICES, OBS_DEV), 1.5, 8.0, ((0, 32),), jnp.float32),
        "obs_var": jnp.clip(jnp.exp(math.log(8.0) - 2.7725887 * jax.random.uniform(key_list[3], (DEVICES, OBS_DEV), jnp.float32) ** steps_of(key_list[3], (DEVICES, OBS_DEV), ((0, 32),), -0.2, 0.2)), 0.5, 8.0),
        "patch_rows": jax.vmap(lambda own: ragged_sizes(own, PATCH_DEV, NLAT, NLAT - NLAT // 4, 0))(jax.random.split(key_list[4], DEVICES)).reshape((DEVICES, PATCH_DEV)).astype(jnp.int32),
    }


lat_coeff = 0.4
lon_coeff = 0.05
advect_coeff = 0.1

def matmul(left, right):
    return jnp.dot(left, right, precision=lax.Precision.HIGHEST, preferred_element_type=jnp.float32)

def advance(padded):
    centre = padded[:, 1:-1]
    northern = padded[:, :-2]
    southern = padded[:, 2:]
    eastern = jnp.roll(centre, -1, axis=2)
    western = jnp.roll(centre, 1, axis=2)
    return centre + lat_coeff * (northern + southern - 2.0 * centre) + lon_coeff * (eastern + western - 2.0 * centre) - advect_coeff * centre * (eastern - western)

def observe(states, cell_index, values):
    observed = jnp.take(states, cell_index, axis=1)
    obs_mean = lax.optimization_barrier(jnp.mean(observed, axis=0))
    return (observed - obs_mean, values - obs_mean)

def localize(obs_rows, rel_cols, first_row, row_count, lat_scale, width_cols):
    lower = first_row.astype(jnp.float32)
    upper = lower + row_count.astype(jnp.float32) - 1.0
    lat_gap = jnp.maximum(jnp.maximum(lower - obs_rows, obs_rows - upper), 0.0) / lat_scale
    lon_gap = jnp.maximum(jnp.maximum(-rel_cols, rel_cols - (width_cols - 1.0)), 0.0) / width_cols
    return jnp.exp(-lat_gap * lat_gap - lon_gap * lon_gap)

def inverse_root(gram_matrix):
    bound = jnp.max(lax.optimization_barrier(jnp.sum(jnp.abs(gram_matrix), axis=1)))
    identity = jnp.eye(gram_matrix.shape[0], dtype=jnp.float32)
    iterate = gram_matrix / bound
    result = identity
    for turn_index in range(NS_ITERS):
        middle = 1.5 * identity - 0.5 * matmul(result, iterate)
        result = matmul(middle, result)
        if turn_index + 1 < NS_ITERS:
            iterate = matmul(iterate, middle)
    return result / jnp.sqrt(bound)

def analyse(states, spread, obs_meta, lengths, width_cols):
    members = states.shape[0]
    cell_total = states.shape[1]
    lat_total = cell_total // width_cols
    state_mean = lax.optimization_barrier(jnp.mean(states, axis=0))
    anomaly = states - state_mean
    starts = jnp.cumsum(lengths) - lengths
    cell_rows = jnp.arange(cell_total, dtype=jnp.int32) // width_cols
    identity = jnp.eye(members, dtype=jnp.float32)
    result = jnp.broadcast_to(state_mean, states.shape)
    for patch in range(lengths.shape[0]):
        weights = localize(obs_meta[2], obs_meta[3], starts[patch], lengths[patch], lat_total / 4.0, float(width_cols)) / obs_meta[1]
        weighted = spread * weights
        gram_matrix = (members - 1.0) * identity + matmul(weighted, spread.T)
        root = inverse_root(gram_matrix)
        drive = matmul(weighted, obs_meta[0])
        mean_weights = matmul(root, matmul(root, drive))
        transform = jnp.sqrt(members - 1.0) * root + mean_weights[:, None]
        update = matmul(transform.T, anomaly)
        cell_mask = (cell_rows >= starts[patch]) & (cell_rows < starts[patch] + lengths[patch])
        result = result + jnp.where(cell_mask[None, :], update, 0.0)
    return result

def reference(ensemble, obs_cell, obs_value, obs_var, patch_rows):
    fields = ensemble
    for _ in range(STEPS):
        fields = advance(jnp.pad(fields, ((0, 0), (1, 1), (0, 0))))
    servers = NLON // LON_DEV
    strips = fields.reshape(K, NLAT, servers, LON_DEV).transpose(2, 0, 1, 3).reshape(servers, K, NLAT * LON_DEV)

    def prepare(server):
        return observe(strips[server], obs_cell[server], obs_value[server])
    spreads, innovs = lax.map(prepare, jnp.arange(servers, dtype=jnp.int32))
    obs_rows = (obs_cell // LON_DEV).astype(jnp.float32)
    obs_cols = (obs_cell % LON_DEV).astype(jnp.float32)
    offsets = jnp.array([-1.0, 0.0, 1.0], jnp.float32)[:, None] * LON_DEV

    def solve(server):
        beside_all = jnp.stack([(server - 1) % servers, server, (server + 1) % servers]).astype(jnp.int32)
        near_spread = spreads[beside_all].transpose(1, 0, 2).reshape(K, 3 * OBS_DEV)
        obs_meta = jnp.stack([innovs[beside_all].reshape(-1), obs_var[beside_all].reshape(-1), obs_rows[beside_all].reshape(-1), (obs_cols[beside_all] + offsets).reshape(-1)])
        return analyse(strips[server], near_spread, obs_meta, patch_rows[server], LON_DEV)
    analysed = lax.map(solve, jnp.arange(servers, dtype=jnp.int32))
    return analysed.reshape(servers, K, NLAT, LON_DEV).transpose(1, 2, 0, 3).reshape(K, NLAT, NLON)
```

```python
import jax
import jax.numpy as jnp
from jax import lax
from jax.sharding import PartitionSpec as P

STEPS = 4


lat_coeff = 0.4
lon_coeff = 0.05
advect_coeff = 0.1


def with_halo(value, sides, width, wrap):
    for axis, dim in sides:
        size, length = (lax.axis_size(axis), value.shape[dim])
        up = [(i, (i + 1) % size) for i in range(size if wrap else size - 1)]
        down = [(j, i) for i, j in up]
        last = lax.slice_in_dim(value, length - width, length, axis=dim)
        initial = lax.slice_in_dim(value, 0, width, axis=dim)
        before = lax.ppermute(last, axis, up)
        after = lax.ppermute(initial, axis, down)
        value = jnp.concatenate([before, value, after], axis=dim)
    return value


def advance(padded):
    centre = padded[:, 1:-1]
    northern = padded[:, :-2]
    southern = padded[:, 2:]
    eastern = jnp.roll(centre, -1, axis=2)
    western = jnp.roll(centre, 1, axis=2)
    return (
        centre
        + lat_coeff * (northern + southern - 2.0 * centre)
        + lon_coeff * (eastern + western - 2.0 * centre)
        - advect_coeff * centre * (eastern - western)
    )


def observe(states, cell_index, values):
    observed = jnp.take(states, cell_index, axis=1)
    obs_mean = jnp.mean(observed, axis=0)
    return (observed - obs_mean, values - obs_mean)


def localize(obs_rows, rel_cols, first_row, row_count, lat_scale, width_cols):
    lower = first_row.astype(jnp.float32)
    upper = lower + row_count.astype(jnp.float32) - 1.0
    lat_gap = jnp.maximum(jnp.maximum(lower - obs_rows, obs_rows - upper), 0.0) / lat_scale
    lon_gap = jnp.maximum(jnp.maximum(-rel_cols, rel_cols - (width_cols - 1.0)), 0.0) / width_cols
    return jnp.exp(-lat_gap * lat_gap - lon_gap * lon_gap)


def dot3(left, right):
    return jnp.matmul(left, right, precision=lax.Precision.HIGH, preferred_element_type=jnp.float32)


def analyse(states, spread, obs_meta, lengths, width_cols):
    members = states.shape[0]
    cell_total = states.shape[1]
    lat_total = cell_total // width_cols
    near = spread.shape[1]
    state_mean = jnp.mean(states, axis=0)
    anomaly = states - state_mean
    starts = jnp.cumsum(lengths) - lengths
    cell_rows = jnp.arange(cell_total, dtype=jnp.int32) // width_cols
    identity = jnp.eye(members, dtype=jnp.float32)
    products = dot3(spread.T, jnp.concatenate([spread, anomaly], axis=1))
    common, crossed = products[:, :near], products[:, near:]
    innov = obs_meta[0]
    shrink = jnp.zeros((cell_total,), jnp.float32)
    shift = state_mean
    weights_all = jnp.zeros((near, cell_total), jnp.float32)
    for patch in range(lengths.shape[0]):
        weights = (
            localize(
                obs_meta[2],
                obs_meta[3],
                starts[patch],
                lengths[patch],
                lat_total / 4.0,
                float(width_cols),
            )
            / obs_meta[1]
        )
        scale = jnp.sqrt(weights)
        gram_matrix = (members - 1.0) * identity + jnp.dot(
            spread * weights, spread.T, preferred_element_type=jnp.float32
        )
        bound = jnp.max(jnp.sum(jnp.abs(gram_matrix), axis=1))
        alpha = (members - 1.0) / bound
        x = common * scale[:, None] * (scale / bound)[None, :]
        c0 = 2.25 + alpha * (-2.4375 + alpha * (1.6875 + alpha * (-0.5625 + alpha * 0.0625)))
        c1 = -2.4375 + alpha * (3.375 + alpha * (-1.6875 + alpha * 0.25))
        c2 = 1.6875 + alpha * (-1.6875 + alpha * 0.375)
        c3 = -0.5625 + alpha * 0.25
        c4 = 0.0625
        x2 = dot3(x, x)
        x34 = dot3(x2, jnp.concatenate([x, x2], axis=1))
        x3, x4 = x34[:, :near], x34[:, near:]
        low = c2 * x + c3 * x2 + c4 * x3
        high = c1 * x + c2 * x2 + c3 * x3 + c4 * x4
        block = jnp.concatenate([crossed * scale[:, None], (scale * innov)[:, None]], axis=1)
        both = dot3(jnp.concatenate([low, high], axis=0), block)
        b1 = c1 * block + both[:near]
        b2 = c0 * block + both[near:]
        b3 = c0 * b2 + dot3(high, b2)
        mixed = alpha * c0 * b1 + b3
        got = 1.5 * b1 - 0.5 * (
            alpha * c0 * c0 * b1
            + c0 * mixed
            + dot3(high, mixed)
            + alpha * (c1 * b3 + dot3(low, b3))
        )
        base = c0 * (1.5 - 0.5 * alpha * c0 * c0)
        driven = base * block[:, -1] + jnp.sum(x * got[:, -1][None, :], axis=1)
        again = jnp.sum(x * driven[None, :], axis=1)
        mean_part = (
            jnp.sum(block[:, :-1] * (base * driven)[:, None] + got[:, :-1] * again[:, None], axis=0)
            / bound
        )
        cell_mask = (cell_rows >= starts[patch]) & (cell_rows < starts[patch] + lengths[patch])
        root_scale = jnp.sqrt((members - 1.0) / bound)
        shift = shift + jnp.where(cell_mask, mean_part, 0.0)
        shrink = jnp.where(cell_mask, root_scale * base, shrink)
        weights_all = jnp.where(
            cell_mask[None, :], got[:, :-1] * (scale * (root_scale / bound))[:, None], weights_all
        )
    return shift + shrink * anomaly + dot3(spread, weights_all)


def per_device(ensemble, obs_cell, obs_value, obs_var, patch_rows):
    fields = ensemble
    members_dev = fields.shape[0]
    lat_rows = fields.shape[1]
    lon_cells = fields.shape[2]
    lat_count = lax.axis_size("lat")
    member_count = lax.axis_size("member")
    servers = lat_count * member_count
    width_cols = lon_cells // servers
    padded = with_halo(fields, (("lat", 1),), STEPS, False)
    global_rows = (
        lax.axis_index("lat") * lat_rows + jnp.arange(lat_rows + 2 * STEPS, dtype=jnp.int32) - STEPS
    )
    inside = ((global_rows >= 0) & (global_rows < lat_rows * lat_count)).astype(jnp.float32)
    for step_index in range(STEPS):
        padded = advance(padded)
        keeper = inside[step_index + 1 : inside.shape[0] - step_index - 1]
        padded = padded * keeper[None, :, None]
    fields = padded
    blocks = fields.reshape(1, members_dev, lat_rows, lon_cells)
    received = lax.all_to_all(blocks, ("member", "lat"), split_axis=3, concat_axis=0, tiled=True)
    strip = received.reshape(member_count, lat_count, members_dev, lat_rows, width_cols)
    strip = strip.transpose(0, 2, 1, 3, 4).reshape(
        member_count * members_dev, lat_count * lat_rows, width_cols
    )
    members = strip.shape[0]
    lat_total = strip.shape[1]
    states = strip.reshape(members, lat_total * width_cols)
    cell_index = obs_cell[0]
    obs_count = cell_index.shape[0]
    spread, innov = observe(states, cell_index, obs_value[0])
    obs_meta = jnp.stack(
        [
            innov,
            obs_var[0],
            (cell_index // width_cols).astype(jnp.float32),
            (cell_index % width_cols).astype(jnp.float32),
        ]
    )
    near_spread, near_meta = (
        with_halo(spread, ((("member", "lat"), 1),), obs_count, True),
        with_halo(obs_meta, ((("member", "lat"), 1),), obs_count, True),
    )
    shifts = jnp.repeat(jnp.array([-1.0, 0.0, 1.0], jnp.float32), obs_count) * width_cols
    near_meta = jnp.concatenate([near_meta[:3], (near_meta[3] + shifts)[None, :]], axis=0)
    analysed = analyse(states, near_spread, near_meta, patch_rows[0], width_cols)
    analysed = analysed.reshape(members, lat_total, width_cols)
    outgoing = analysed.reshape(member_count, members_dev, lat_count, lat_rows, width_cols)
    outgoing = outgoing.transpose(0, 2, 1, 3, 4).reshape(servers, members_dev, lat_rows, width_cols)
    returned = lax.all_to_all(outgoing, ("member", "lat"), split_axis=0, concat_axis=3, tiled=True)
    return returned.reshape(members_dev, lat_rows, lon_cells)


def solution(mesh):
    in_specs = (
        P("member", "lat", None),
        P(("member", "lat"), None),
        P(("member", "lat"), None),
        P(("member", "lat"), None),
        P(("member", "lat"), None),
    )
    out_specs = P("member", "lat", None)
    return jax.shard_map(
        per_device, mesh=mesh, in_specs=in_specs, out_specs=out_specs, check_vma=False
    )
```

```python
import functools

import jax
import jax.numpy as jnp
from jax import lax
from jax.experimental import pallas as pl
from jax.experimental.pallas import tpu as pltpu
from jax.sharding import PartitionSpec as P

STEPS = 4


lat_coeff = 0.4
lon_coeff = 0.05
advect_coeff = 0.1


def with_halo(value, sides, width, wrap):
    for axis, dim in sides:
        size, length = (lax.axis_size(axis), value.shape[dim])
        up = [(i, (i + 1) % size) for i in range(size if wrap else size - 1)]
        down = [(j, i) for i, j in up]
        last = lax.slice_in_dim(value, length - width, length, axis=dim)
        initial = lax.slice_in_dim(value, 0, width, axis=dim)
        before = lax.ppermute(last, axis, up)
        after = lax.ppermute(initial, axis, down)
        value = jnp.concatenate([before, value, after], axis=dim)
    return value


def advance(padded):
    centre = padded[:, 1:-1]
    northern = padded[:, :-2]
    southern = padded[:, 2:]
    eastern = jnp.roll(centre, -1, axis=2)
    western = jnp.roll(centre, 1, axis=2)
    return (
        centre
        + lat_coeff * (northern + southern - 2.0 * centre)
        + lon_coeff * (eastern + western - 2.0 * centre)
        - advect_coeff * centre * (eastern - western)
    )


def observe(states, cell_index, values):
    observed = jnp.take(states, cell_index, axis=1)
    obs_mean = jnp.mean(observed, axis=0)
    return (observed - obs_mean, values - obs_mean)


def localize(obs_rows, rel_cols, first_row, row_count, lat_scale, width_cols):
    lower = first_row.astype(jnp.float32)
    upper = lower + row_count.astype(jnp.float32) - 1.0
    lat_gap = jnp.maximum(jnp.maximum(lower - obs_rows, obs_rows - upper), 0.0) / lat_scale
    lon_gap = jnp.maximum(jnp.maximum(-rel_cols, rel_cols - (width_cols - 1.0)), 0.0) / width_cols
    return jnp.exp(-lat_gap * lat_gap - lon_gap * lon_gap)


def dot3(left, right):
    return jnp.matmul(left, right, precision=lax.Precision.HIGH, preferred_element_type=jnp.float32)


def analyse(states, spread, obs_meta, lengths, width_cols):
    members = states.shape[1]
    cell_total = states.shape[0]
    lat_total = cell_total // width_cols
    near = spread.shape[0]
    state_mean = jnp.mean(states, axis=1)
    anomaly = states - state_mean[:, None]
    starts = jnp.cumsum(lengths) - lengths
    cell_rows = jnp.arange(cell_total, dtype=jnp.int32) // width_cols
    identity = jnp.eye(members, dtype=jnp.float32)
    products = dot3(spread, jnp.concatenate([spread, anomaly], axis=0).T)
    common, crossed = products[:, :near], products[:, near:]
    innov = obs_meta[0]
    shrink = jnp.zeros((cell_total,), jnp.float32)
    shift = state_mean
    weights_all = jnp.zeros((near, cell_total), jnp.float32)
    for patch in range(lengths.shape[0]):
        weights = (
            localize(
                obs_meta[2],
                obs_meta[3],
                starts[patch],
                lengths[patch],
                lat_total / 4.0,
                float(width_cols),
            )
            / obs_meta[1]
        )
        scale = jnp.sqrt(weights)
        gram_matrix = (members - 1.0) * identity + jnp.dot(
            (spread * weights[:, None]).T, spread, preferred_element_type=jnp.float32
        )
        bound = jnp.max(jnp.sum(jnp.abs(gram_matrix), axis=1))
        alpha = (members - 1.0) / bound
        x = common * scale[:, None] * (scale / bound)[None, :]
        c0 = 2.25 + alpha * (-2.4375 + alpha * (1.6875 + alpha * (-0.5625 + alpha * 0.0625)))
        c1 = -2.4375 + alpha * (3.375 + alpha * (-1.6875 + alpha * 0.25))
        c2 = 1.6875 + alpha * (-1.6875 + alpha * 0.375)
        c3 = -0.5625 + alpha * 0.25
        c4 = 0.0625
        x2 = dot3(x, x)
        x34 = dot3(x2, jnp.concatenate([x, x2], axis=1))
        x3, x4 = x34[:, :near], x34[:, near:]
        low = c2 * x + c3 * x2 + c4 * x3
        high = c1 * x + c2 * x2 + c3 * x3 + c4 * x4
        block = jnp.concatenate([crossed * scale[:, None], (scale * innov)[:, None]], axis=1)
        both = dot3(jnp.concatenate([low, high], axis=0), block)
        b1 = c1 * block + both[:near]
        b2 = c0 * block + both[near:]
        b3 = c0 * b2 + dot3(high, b2)
        mixed = alpha * c0 * b1 + b3
        got = 1.5 * b1 - 0.5 * (
            alpha * c0 * c0 * b1
            + c0 * mixed
            + dot3(high, mixed)
            + alpha * (c1 * b3 + dot3(low, b3))
        )
        base = c0 * (1.5 - 0.5 * alpha * c0 * c0)
        driven = base * block[:, -1] + jnp.sum(x * got[:, -1][None, :], axis=1)
        again = jnp.sum(x * driven[None, :], axis=1)
        mean_part = (
            jnp.sum(block[:, :-1] * (base * driven)[:, None] + got[:, :-1] * again[:, None], axis=0)
            / bound
        )
        cell_mask = (cell_rows >= starts[patch]) & (cell_rows < starts[patch] + lengths[patch])
        root_scale = jnp.sqrt((members - 1.0) / bound)
        shift = shift + jnp.where(cell_mask, mean_part, 0.0)
        shrink = jnp.where(cell_mask, root_scale * base, shrink)
        weights_all = jnp.where(
            cell_mask[None, :], got[:, :-1] * (scale * (root_scale / bound))[:, None], weights_all
        )
    return shift[:, None] + shrink[:, None] * anomaly + dot3(weights_all.T, spread)


def plain_device(ensemble, obs_cell, obs_value, obs_var, patch_rows):
    fields = ensemble
    members_dev = fields.shape[0]
    lat_rows = fields.shape[1]
    lon_cells = fields.shape[2]
    lat_count = lax.axis_size("lat")
    member_count = lax.axis_size("member")
    servers = lat_count * member_count
    width_cols = lon_cells // servers
    padded = with_halo(fields, (("lat", 1),), STEPS, False)
    global_rows = (
        lax.axis_index("lat") * lat_rows + jnp.arange(lat_rows + 2 * STEPS, dtype=jnp.int32) - STEPS
    )
    inside = ((global_rows >= 0) & (global_rows < lat_rows * lat_count)).astype(jnp.float32)
    for step_index in range(STEPS):
        padded = advance(padded)
        keeper = inside[step_index + 1 : inside.shape[0] - step_index - 1]
        padded = padded * keeper[None, :, None]
    fields = padded
    blocks = fields.reshape(1, members_dev, lat_rows, lon_cells)
    received = lax.all_to_all(blocks, ("member", "lat"), split_axis=3, concat_axis=0, tiled=True)
    strip = received.reshape(member_count, lat_count, members_dev, lat_rows, width_cols)
    strip = strip.transpose(0, 2, 1, 3, 4).reshape(
        member_count * members_dev, lat_count * lat_rows, width_cols
    )
    members = strip.shape[0]
    lat_total = strip.shape[1]
    states = strip.reshape(members, lat_total * width_cols)
    cell_index = obs_cell[0]
    obs_count = cell_index.shape[0]
    spread, innov = observe(states, cell_index, obs_value[0])
    obs_meta = jnp.stack(
        [
            innov,
            obs_var[0],
            (cell_index // width_cols).astype(jnp.float32),
            (cell_index % width_cols).astype(jnp.float32),
        ]
    )
    near_spread, near_meta = (
        with_halo(spread, ((("member", "lat"), 1),), obs_count, True),
        with_halo(obs_meta, ((("member", "lat"), 1),), obs_count, True),
    )
    shifts = jnp.repeat(jnp.array([-1.0, 0.0, 1.0], jnp.float32), obs_count) * width_cols
    near_meta = jnp.concatenate([near_meta[:3], (near_meta[3] + shifts)[None, :]], axis=0)
    analysed = analyse(states.T, near_spread.T, near_meta, patch_rows[0], width_cols).T
    analysed = analysed.reshape(members, lat_total, width_cols)
    outgoing = analysed.reshape(member_count, members_dev, lat_count, lat_rows, width_cols)
    outgoing = outgoing.transpose(0, 2, 1, 3, 4).reshape(servers, members_dev, lat_rows, width_cols)
    returned = lax.all_to_all(outgoing, ("member", "lat"), split_axis=0, concat_axis=3, tiled=True)
    return returned.reshape(members_dev, lat_rows, lon_cells)


LANES = 128


def group_of(place):
    return place + (place % 4) // 2 * (1 - 2 * (place % 2))


def turn_of(group, index, size):
    return (group % 2) * (size - 1 - index) + (1 - group % 2) * index


def server_of(member, lat, member_count):
    group = group_of(lat)
    return member_count * group + turn_of(group, member, member_count)


def host_of(server, member_count):
    group = server // member_count
    return turn_of(group, server % member_count, member_count), group_of(group)


def exchange_kernel(count, place, source, target, me_of, x_ref, o_ref, send_sem, recv_sem, own_sem):
    me = me_of()
    barrier = pltpu.get_barrier_semaphore()

    def greet(step, carry):
        pl.semaphore_signal(barrier, inc=1, device_id=place(lax.rem(me + step, count)), device_id_type=pl.DeviceIdType.MESH)
        return carry

    lax.fori_loop(1, count, greet, 0)
    own = pltpu.make_async_copy(x_ref.at[source(me)], o_ref.at[target(me)], own_sem)
    own.start()
    pl.semaphore_wait(barrier, count - 1)

    def sending(step):
        other = lax.rem(me + step, count)
        return pltpu.make_async_remote_copy(
            src_ref=x_ref.at[source(other)],
            dst_ref=o_ref.at[target(me)],
            send_sem=send_sem.at[step],
            recv_sem=recv_sem.at[step],
            device_id=place(other),
            device_id_type=pl.DeviceIdType.MESH,
        )

    def arriving(step):
        other = lax.rem(me + count - step, count)
        return pltpu.make_async_remote_copy(
            src_ref=x_ref.at[source(other)],
            dst_ref=o_ref.at[target(other)],
            send_sem=send_sem.at[step],
            recv_sem=recv_sem.at[step],
            device_id=place(other),
            device_id_type=pl.DeviceIdType.MESH,
        )

    def start(step, carry):
        sending(step).start()
        return carry

    def finish(step, carry):
        arriving(step).wait_recv()
        sending(step).wait_send()
        return carry

    lax.fori_loop(1, count, start, 0)
    own.wait()
    lax.fori_loop(1, count, finish, 0)


def exchange(blocks, count, place, source, target, me_of, number):
    moved = blocks.size * 4
    return pl.pallas_call(
        functools.partial(exchange_kernel, count, place, source, target, me_of),
        out_shape=jax.ShapeDtypeStruct(blocks.shape, jnp.float32),
        in_specs=[pl.BlockSpec(memory_space=pltpu.VMEM)],
        out_specs=pl.BlockSpec(memory_space=pltpu.VMEM),
        scratch_shapes=[
            pltpu.SemaphoreType.DMA((count,)),
            pltpu.SemaphoreType.DMA((count,)),
            pltpu.SemaphoreType.DMA,
        ],
        compiler_params=pltpu.CompilerParams(collective_id=number, has_side_effects=True),
        cost_estimate=pl.CostEstimate(flops=0, bytes_accessed=40 * moved, transcendentals=0),
    )(blocks)


def ring_kernel(member_count, lat_count, x_ref, before_ref, after_ref, send_sem, recv_sem):
    servers = member_count * lat_count
    me = server_of(lax.axis_index("member"), lax.axis_index("lat"), member_count)

    def place(server):
        member, lat = host_of(server, member_count)
        return {"member": member, "lat": lat}

    up, down = place(lax.rem(me + 1, servers)), place(lax.rem(me + servers - 1, servers))
    barrier = pltpu.get_barrier_semaphore()
    for beside in (up, down):
        pl.semaphore_signal(barrier, inc=1, device_id=beside, device_id_type=pl.DeviceIdType.MESH)
    pl.semaphore_wait(barrier, 2)
    copies = []
    for side, (beside, landing) in enumerate(((up, before_ref), (down, after_ref))):
        copy = pltpu.make_async_remote_copy(
            src_ref=x_ref,
            dst_ref=landing,
            send_sem=send_sem.at[side],
            recv_sem=recv_sem.at[side],
            device_id=beside,
            device_id_type=pl.DeviceIdType.MESH,
        )
        copy.start()
        copies.append(copy)
    for copy in copies:
        copy.wait()


def ring(own, member_count, lat_count, number):
    shape = jax.ShapeDtypeStruct(own.shape, jnp.float32)
    vmem = pl.BlockSpec(memory_space=pltpu.VMEM)
    return pl.pallas_call(
        functools.partial(ring_kernel, member_count, lat_count),
        out_shape=(shape, shape),
        in_specs=[vmem],
        out_specs=(vmem, vmem),
        scratch_shapes=[pltpu.SemaphoreType.DMA((2,)), pltpu.SemaphoreType.DMA((2,))],
        compiler_params=pltpu.CompilerParams(collective_id=number, has_side_effects=True),
        cost_estimate=pl.CostEstimate(flops=0, bytes_accessed=100 * own.size, transcendentals=0),
    )(own)


def forecast_kernel(strips, width_cols, x_ref, o_ref):
    lat_count, packed, cells, _ = x_ref.shape
    lat_rows = packed - 1
    piece = LANES // lat_rows
    main = x_ref[:, :lat_rows].reshape(lat_count * lat_rows, cells, LANES)
    rest = x_ref[:, lat_rows]
    lane = lax.broadcasted_iota(jnp.int32, rest.shape, 2)

    def step(centre, north, south):
        east = pltpu.roll(centre, cells - 1, axis=1)
        west = pltpu.roll(centre, 1, axis=1)
        return (
            centre
            + lat_coeff * (north + south - 2.0 * centre)
            + lon_coeff * (east + west - 2.0 * centre)
            - advect_coeff * centre * (east - west)
        )

    empty = jnp.zeros((1, cells, LANES), jnp.float32)
    for _ in range(STEPS):
        main_north = jnp.concatenate([empty, main[:-1]], axis=0)
        main_south = jnp.concatenate([main[1:], empty], axis=0)
        lower = pltpu.roll(rest, piece, axis=2)
        upper = pltpu.roll(rest, LANES - piece, axis=2)
        rest_north = jnp.where(lane < piece, jnp.concatenate([empty, lower[:-1]], axis=0), lower)
        rest_south = jnp.where(lane >= LANES - piece, jnp.concatenate([upper[1:], empty], axis=0), upper)
        main = step(main, main_north, main_south)
        rest = step(rest, rest_north, rest_south)
    main = pltpu.roll(main, cells - STEPS, axis=1)
    rest = pltpu.roll(rest, cells - STEPS, axis=1)
    for strip in range(strips):
        own = slice(strip * width_cols, (strip + 1) * width_cols)
        o_ref[strip, :, :lat_rows] = main[:, own].reshape(lat_count, lat_rows, width_cols, LANES)
        o_ref[strip, :, lat_rows] = rest[:, own]


def gather_kernel(x_ref, o_ref):
    member_count, lat_count, packed, width_cols, _ = x_ref.shape
    lat_rows = packed - 1
    piece = LANES // lat_rows
    cells = lat_count * lat_rows * width_cols
    for member in range(member_count):
        o_ref[:, member * LANES : (member + 1) * LANES] = x_ref[member, :, :lat_rows].reshape(cells, LANES)
    rest = [x_ref[member, :, lat_rows] for member in range(member_count)]
    part = lax.broadcasted_iota(jnp.int32, rest[0].shape, 2) // piece
    rows = []
    for row in range(lat_rows):
        total = rest[row]
        for member in range(member_count):
            if member != row:
                moved = pltpu.roll(rest[member], (member - row) * piece % LANES, axis=2)
                total = jnp.where(part == member, moved, total)
        rows.append(total)
    o_ref[:, member_count * LANES :] = jnp.stack(rows, axis=1).reshape(cells, LANES)


def scatter_kernel(lat_count, width_cols, x_ref, o_ref):
    member_count = x_ref.shape[1] // LANES - 1
    lat_rows = o_ref.shape[1] - 1
    piece = LANES // lat_rows
    held = x_ref[:, member_count * LANES :].reshape(lat_count, lat_rows, width_cols, LANES)
    part = lax.broadcasted_iota(jnp.int32, held[:, 0].shape, 2) // piece
    for member in range(member_count):
        own = slice(member * lat_count, (member + 1) * lat_count)
        o_ref[own, :lat_rows] = x_ref[:, member * LANES : (member + 1) * LANES].reshape(
            lat_count, lat_rows, width_cols, LANES
        )
        total = held[:, member]
        for row in range(lat_rows):
            if row != member:
                moved = pltpu.roll(held[:, row], (row - member) * piece % LANES, axis=2)
                total = jnp.where(part == row, moved, total)
        o_ref[own, lat_rows] = total


def local(kernel, shape, *operands):
    vmem = pl.BlockSpec(memory_space=pltpu.VMEM)
    return pl.pallas_call(
        kernel,
        out_shape=jax.ShapeDtypeStruct(shape, jnp.float32),
        in_specs=[vmem] * len(operands),
        out_specs=vmem,
        cost_estimate=pl.CostEstimate(flops=10**6, bytes_accessed=10**7, transcendentals=0),
    )(*operands)


def packed_device(ensemble, obs_cell, obs_value, obs_var, patch_rows):
    members_dev, lat_rows, lon_cells = ensemble.shape
    lat_count, member_count = lax.axis_size("lat"), lax.axis_size("member")
    servers = lat_count * member_count
    width_cols = lon_cells // servers
    span = lon_cells // lat_count
    obs_count = obs_cell.shape[1]
    patches = patch_rows.shape[1]

    meta = jnp.concatenate(
        [
            obs_value,
            obs_var,
            obs_cell.astype(jnp.float32),
            jnp.pad(patch_rows.astype(jnp.float32), ((0, 0), (0, obs_count - patches))),
        ],
        axis=0,
    )
    near_meta = []
    for offset in (-1, 0, 1):
        pairs = []
        for server in range(servers):
            member, lat = host_of(server, member_count)
            pairs.append(((server + offset) % servers, member * lat_count + lat))
        near_meta.append(lax.ppermute(meta, ("member", "lat"), pairs))

    cells = ensemble.transpose(1, 2, 0)
    piece = members_dev - LANES
    rest = cells[:, :, LANES:].transpose(1, 0, 2).reshape(1, lon_cells, lat_rows * piece)
    packed = jnp.concatenate([cells[:, :, :LANES], rest], axis=0)
    wide = jnp.concatenate([packed[:, -STEPS:], packed, packed[:, :STEPS]], axis=1)
    outgoing = jnp.stack(
        [
            wide[:, group_of(lat) * span : group_of(lat) * span + span + 2 * STEPS]
            for lat in range(lat_count)
        ]
    )
    got = exchange(
        outgoing,
        lat_count,
        lambda p: {"lat": p},
        lambda p: p,
        lambda p: p,
        lambda: lax.axis_index("lat"),
        1,
    )
    strips = local(
        functools.partial(forecast_kernel, member_count, width_cols),
        (member_count, lat_count, lat_rows + 1, width_cols, LANES),
        got,
    )
    got = exchange(
        strips,
        member_count,
        lambda p: {"member": p},
        lambda p: turn_of(group_of(lax.axis_index("lat")), p, member_count),
        lambda p: p,
        lambda: lax.axis_index("member"),
        2,
    )
    states = local(gather_kernel, (lat_count * lat_rows * width_cols, members_dev * member_count), got)
    observed = jnp.take(states, near_meta[1][2].astype(jnp.int32), axis=0)
    before, after = ring(observed, member_count, lat_count, 3)
    near = jnp.concatenate([before, observed, after], axis=0)
    near_mean = jnp.mean(near, axis=1)
    spread = near - near_mean[:, None]
    joined = jnp.concatenate(near_meta, axis=1)
    places = joined[2].astype(jnp.int32)
    shifts = jnp.repeat(jnp.array([-1.0, 0.0, 1.0], jnp.float32), obs_count) * width_cols
    obs_meta = (
        joined[0] - near_mean,
        joined[1],
        (places // width_cols).astype(jnp.float32),
        (places % width_cols).astype(jnp.float32) + shifts,
    )
    lengths = near_meta[1][3, :patches].astype(jnp.int32)
    analysed = analyse(states, spread, obs_meta, lengths, width_cols)
    outgoing = local(
        functools.partial(scatter_kernel, lat_count, width_cols),
        (servers, lat_rows + 1, width_cols, LANES),
        analysed,
    )
    got = exchange(
        outgoing,
        servers,
        lambda p: {"member": p // lat_count, "lat": p % lat_count},
        lambda p: p,
        lambda p: server_of(p // lat_count, p % lat_count, member_count),
        lambda: lax.axis_index("member") * lat_count + lax.axis_index("lat"),
        4,
    )
    main = got[:, :lat_rows].transpose(3, 1, 0, 2).reshape(LANES, lat_rows, lon_cells)
    rest = got[:, lat_rows].reshape(lon_cells, lat_rows, piece).transpose(2, 1, 0)
    return jnp.concatenate([main, rest], axis=0)


def per_device(ensemble, obs_cell, obs_value, obs_var, patch_rows):
    members_dev, lat_rows, lon_cells = ensemble.shape
    lat_count, member_count = lax.axis_size("lat"), lax.axis_size("member")
    fits = (
        (members_dev - LANES) * lat_rows == LANES
        and member_count == lat_rows
        and lat_count % 4 == 0
        and lon_cells // (lat_count * member_count) == 8
        and STEPS == 4
        and patch_rows.shape[1] <= obs_cell.shape[1]
    )
    device = packed_device if fits else plain_device
    return device(ensemble, obs_cell, obs_value, obs_var, patch_rows)


def solution(mesh):
    in_specs = (
        P("member", "lat", None),
        P(("member", "lat"), None),
        P(("member", "lat"), None),
        P(("member", "lat"), None),
        P(("member", "lat"), None),
    )
    out_specs = P("member", "lat", None)
    return jax.shard_map(
        per_device, mesh=mesh, in_specs=in_specs, out_specs=out_specs, check_vma=False
    )
```

```python
import functools

import jax
import jax.numpy as jnp
from jax import lax
from jax.experimental import pallas as pl
from jax.experimental.pallas import tpu as pltpu
from jax.sharding import PartitionSpec as P

STEPS = 4


lat_coeff = 0.4
lon_coeff = 0.05
advect_coeff = 0.1


def with_halo(value, sides, width, wrap):
    for axis, dim in sides:
        size, length = (lax.axis_size(axis), value.shape[dim])
        up = [(i, (i + 1) % size) for i in range(size if wrap else size - 1)]
        down = [(j, i) for i, j in up]
        last = lax.slice_in_dim(value, length - width, length, axis=dim)
        initial = lax.slice_in_dim(value, 0, width, axis=dim)
        before = lax.ppermute(last, axis, up)
        after = lax.ppermute(initial, axis, down)
        value = jnp.concatenate([before, value, after], axis=dim)
    return value


def advance(padded):
    centre = padded[:, 1:-1]
    northern = padded[:, :-2]
    southern = padded[:, 2:]
    eastern = jnp.roll(centre, -1, axis=2)
    western = jnp.roll(centre, 1, axis=2)
    return (
        centre
        + lat_coeff * (northern + southern - 2.0 * centre)
        + lon_coeff * (eastern + western - 2.0 * centre)
        - advect_coeff * centre * (eastern - western)
    )


def observe(states, cell_index, values):
    observed = jnp.take(states, cell_index, axis=1)
    obs_mean = jnp.mean(observed, axis=0)
    return (observed - obs_mean, values - obs_mean)


def localize(obs_rows, rel_cols, first_row, row_count, lat_scale, width_cols):
    lower = first_row.astype(jnp.float32)
    upper = lower + row_count.astype(jnp.float32) - 1.0
    lat_gap = jnp.maximum(jnp.maximum(lower - obs_rows, obs_rows - upper), 0.0) / lat_scale
    lon_gap = jnp.maximum(jnp.maximum(-rel_cols, rel_cols - (width_cols - 1.0)), 0.0) / width_cols
    return jnp.exp(-lat_gap * lat_gap - lon_gap * lon_gap)


def dot3(left, right):
    return jnp.matmul(left, right, precision=lax.Precision.HIGH, preferred_element_type=jnp.float32)


def analyse(states, spread, obs_meta, lengths, width_cols):
    members = states.shape[1]
    cell_total = states.shape[0]
    lat_total = cell_total // width_cols
    near = spread.shape[0]
    state_mean = jnp.mean(states, axis=1)
    anomaly = states - state_mean[:, None]
    starts = jnp.cumsum(lengths) - lengths
    cell_rows = jnp.arange(cell_total, dtype=jnp.int32) // width_cols
    identity = jnp.eye(members, dtype=jnp.float32)
    products = dot3(spread, jnp.concatenate([spread, anomaly], axis=0).T)
    common, crossed = products[:, :near], products[:, near:]
    innov = obs_meta[0]
    shrink = jnp.zeros((cell_total,), jnp.float32)
    shift = state_mean
    weights_all = jnp.zeros((near, cell_total), jnp.float32)
    for patch in range(lengths.shape[0]):
        weights = (
            localize(
                obs_meta[2],
                obs_meta[3],
                starts[patch],
                lengths[patch],
                lat_total / 4.0,
                float(width_cols),
            )
            / obs_meta[1]
        )
        scale = jnp.sqrt(weights)
        gram_matrix = (members - 1.0) * identity + jnp.dot(
            (spread * weights[:, None]).T, spread, preferred_element_type=jnp.float32
        )
        bound = jnp.max(jnp.sum(jnp.abs(gram_matrix), axis=1))
        alpha = (members - 1.0) / bound
        x = common * scale[:, None] * (scale / bound)[None, :]
        c0 = 2.25 + alpha * (-2.4375 + alpha * (1.6875 + alpha * (-0.5625 + alpha * 0.0625)))
        c1 = -2.4375 + alpha * (3.375 + alpha * (-1.6875 + alpha * 0.25))
        c2 = 1.6875 + alpha * (-1.6875 + alpha * 0.375)
        c3 = -0.5625 + alpha * 0.25
        c4 = 0.0625
        x2 = dot3(x, x)
        x34 = dot3(x2, jnp.concatenate([x, x2], axis=1))
        x3, x4 = x34[:, :near], x34[:, near:]
        low = c2 * x + c3 * x2 + c4 * x3
        high = c1 * x + c2 * x2 + c3 * x3 + c4 * x4
        block = jnp.concatenate([crossed * scale[:, None], (scale * innov)[:, None]], axis=1)
        both = dot3(jnp.concatenate([low, high], axis=0), block)
        b1 = c1 * block + both[:near]
        b2 = c0 * block + both[near:]
        b3 = c0 * b2 + dot3(high, b2)
        mixed = alpha * c0 * b1 + b3
        got = 1.5 * b1 - 0.5 * (
            alpha * c0 * c0 * b1
            + c0 * mixed
            + dot3(high, mixed)
            + alpha * (c1 * b3 + dot3(low, b3))
        )
        base = c0 * (1.5 - 0.5 * alpha * c0 * c0)
        driven = base * block[:, -1] + jnp.sum(x * got[:, -1][None, :], axis=1)
        again = jnp.sum(x * driven[None, :], axis=1)
        mean_part = (
            jnp.sum(block[:, :-1] * (base * driven)[:, None] + got[:, :-1] * again[:, None], axis=0)
            / bound
        )
        cell_mask = (cell_rows >= starts[patch]) & (cell_rows < starts[patch] + lengths[patch])
        root_scale = jnp.sqrt((members - 1.0) / bound)
        shift = shift + jnp.where(cell_mask, mean_part, 0.0)
        shrink = jnp.where(cell_mask, root_scale * base, shrink)
        weights_all = jnp.where(
            cell_mask[None, :], got[:, :-1] * (scale * (root_scale / bound))[:, None], weights_all
        )
    return shift[:, None] + shrink[:, None] * anomaly + dot3(weights_all.T, spread)


def plain_device(ensemble, obs_cell, obs_value, obs_var, patch_rows):
    fields = ensemble
    members_dev = fields.shape[0]
    lat_rows = fields.shape[1]
    lon_cells = fields.shape[2]
    lat_count = lax.axis_size("lat")
    member_count = lax.axis_size("member")
    servers = lat_count * member_count
    width_cols = lon_cells // servers
    padded = with_halo(fields, (("lat", 1),), STEPS, False)
    global_rows = (
        lax.axis_index("lat") * lat_rows + jnp.arange(lat_rows + 2 * STEPS, dtype=jnp.int32) - STEPS
    )
    inside = ((global_rows >= 0) & (global_rows < lat_rows * lat_count)).astype(jnp.float32)
    for step_index in range(STEPS):
        padded = advance(padded)
        keeper = inside[step_index + 1 : inside.shape[0] - step_index - 1]
        padded = padded * keeper[None, :, None]
    fields = padded
    blocks = fields.reshape(1, members_dev, lat_rows, lon_cells)
    received = lax.all_to_all(blocks, ("member", "lat"), split_axis=3, concat_axis=0, tiled=True)
    strip = received.reshape(member_count, lat_count, members_dev, lat_rows, width_cols)
    strip = strip.transpose(0, 2, 1, 3, 4).reshape(
        member_count * members_dev, lat_count * lat_rows, width_cols
    )
    members = strip.shape[0]
    lat_total = strip.shape[1]
    states = strip.reshape(members, lat_total * width_cols)
    cell_index = obs_cell[0]
    obs_count = cell_index.shape[0]
    spread, innov = observe(states, cell_index, obs_value[0])
    obs_meta = jnp.stack(
        [
            innov,
            obs_var[0],
            (cell_index // width_cols).astype(jnp.float32),
            (cell_index % width_cols).astype(jnp.float32),
        ]
    )
    near_spread, near_meta = (
        with_halo(spread, ((("member", "lat"), 1),), obs_count, True),
        with_halo(obs_meta, ((("member", "lat"), 1),), obs_count, True),
    )
    shifts = jnp.repeat(jnp.array([-1.0, 0.0, 1.0], jnp.float32), obs_count) * width_cols
    near_meta = jnp.concatenate([near_meta[:3], (near_meta[3] + shifts)[None, :]], axis=0)
    analysed = analyse(states.T, near_spread.T, near_meta, patch_rows[0], width_cols).T
    analysed = analysed.reshape(members, lat_total, width_cols)
    outgoing = analysed.reshape(member_count, members_dev, lat_count, lat_rows, width_cols)
    outgoing = outgoing.transpose(0, 2, 1, 3, 4).reshape(servers, members_dev, lat_rows, width_cols)
    returned = lax.all_to_all(outgoing, ("member", "lat"), split_axis=0, concat_axis=3, tiled=True)
    return returned.reshape(members_dev, lat_rows, lon_cells)


LANES = 128


def group_of(place, size):
    return place % 2 * (size - 1 - place // 2) + (1 - place % 2) * (place // 2)


def place_of(group, size):
    late = group * 2 // size
    return late * (2 * (size - 1 - group) + 1) + (1 - late) * 2 * group


def turn_of(group, index, size):
    return (group % 2) * (size - 1 - index) + (1 - group % 2) * index


def server_of(member, lat, member_count, lat_count):
    group = group_of(lat, lat_count)
    return member_count * group + turn_of(group, member, member_count)


def host_of(server, member_count, lat_count):
    group = server // member_count
    return turn_of(group, server % member_count, member_count), place_of(group, lat_count)


def exchange_kernel(count, place, source, target, me_of, x_ref, o_ref, send_sem, recv_sem, own_sem):
    me = me_of()
    barrier = pltpu.get_barrier_semaphore()

    def greet(step, carry):
        pl.semaphore_signal(barrier, inc=1, device_id=place(lax.rem(me + step, count)), device_id_type=pl.DeviceIdType.MESH)
        return carry

    lax.fori_loop(1, count, greet, 0)
    own = pltpu.make_async_copy(x_ref.at[source(me)], o_ref.at[target(me)], own_sem)
    own.start()
    pl.semaphore_wait(barrier, count - 1)

    def sending(step):
        other = lax.rem(me + step, count)
        return pltpu.make_async_remote_copy(
            src_ref=x_ref.at[source(other)],
            dst_ref=o_ref.at[target(me)],
            send_sem=send_sem.at[step],
            recv_sem=recv_sem.at[step],
            device_id=place(other),
            device_id_type=pl.DeviceIdType.MESH,
        )

    def arriving(step):
        other = lax.rem(me + count - step, count)
        return pltpu.make_async_remote_copy(
            src_ref=x_ref.at[source(other)],
            dst_ref=o_ref.at[target(other)],
            send_sem=send_sem.at[step],
            recv_sem=recv_sem.at[step],
            device_id=place(other),
            device_id_type=pl.DeviceIdType.MESH,
        )

    def start(step, carry):
        sending(step).start()
        return carry

    def finish(step, carry):
        arriving(step).wait_recv()
        sending(step).wait_send()
        return carry

    lax.fori_loop(1, count, start, 0)
    own.wait()
    lax.fori_loop(1, count, finish, 0)


def exchange(blocks, count, place, source, target, me_of, number):
    moved = blocks.size * 4
    return pl.pallas_call(
        functools.partial(exchange_kernel, count, place, source, target, me_of),
        out_shape=jax.ShapeDtypeStruct(blocks.shape, jnp.float32),
        in_specs=[pl.BlockSpec(memory_space=pltpu.VMEM)],
        out_specs=pl.BlockSpec(memory_space=pltpu.VMEM),
        scratch_shapes=[
            pltpu.SemaphoreType.DMA((count,)),
            pltpu.SemaphoreType.DMA((count,)),
            pltpu.SemaphoreType.DMA,
        ],
        compiler_params=pltpu.CompilerParams(collective_id=number, has_side_effects=True),
        cost_estimate=pl.CostEstimate(flops=0, bytes_accessed=40 * moved, transcendentals=0),
    )(blocks)


def ring_kernel(member_count, lat_count, x_ref, before_ref, after_ref, send_sem, recv_sem):
    servers = member_count * lat_count
    me = server_of(lax.axis_index("member"), lax.axis_index("lat"), member_count, lat_count)

    def place(server):
        member, lat = host_of(server, member_count, lat_count)
        return {"member": member, "lat": lat}

    up, down = place(lax.rem(me + 1, servers)), place(lax.rem(me + servers - 1, servers))
    barrier = pltpu.get_barrier_semaphore()
    for beside in (up, down):
        pl.semaphore_signal(barrier, inc=1, device_id=beside, device_id_type=pl.DeviceIdType.MESH)
    pl.semaphore_wait(barrier, 2)
    copies = []
    for side, (beside, landing) in enumerate(((up, before_ref), (down, after_ref))):
        copy = pltpu.make_async_remote_copy(
            src_ref=x_ref,
            dst_ref=landing,
            send_sem=send_sem.at[side],
            recv_sem=recv_sem.at[side],
            device_id=beside,
            device_id_type=pl.DeviceIdType.MESH,
        )
        copy.start()
        copies.append(copy)
    for copy in copies:
        copy.wait()


def ring(own, member_count, lat_count, number):
    shape = jax.ShapeDtypeStruct(own.shape, jnp.float32)
    vmem = pl.BlockSpec(memory_space=pltpu.VMEM)
    return pl.pallas_call(
        functools.partial(ring_kernel, member_count, lat_count),
        out_shape=(shape, shape),
        in_specs=[vmem],
        out_specs=(vmem, vmem),
        scratch_shapes=[pltpu.SemaphoreType.DMA((2,)), pltpu.SemaphoreType.DMA((2,))],
        compiler_params=pltpu.CompilerParams(collective_id=number, has_side_effects=True),
        cost_estimate=pl.CostEstimate(flops=0, bytes_accessed=100 * own.size, transcendentals=0),
    )(own)


def forecast_kernel(strips, width_cols, x_ref, o_ref):
    lat_count, packed, cells, _ = x_ref.shape
    lat_rows = packed - 1
    piece = LANES // lat_rows
    main = x_ref[:, :lat_rows].reshape(lat_count * lat_rows, cells, LANES)
    rest = x_ref[:, lat_rows]
    lane = lax.broadcasted_iota(jnp.int32, rest.shape, 2)

    def step(centre, north, south):
        east = pltpu.roll(centre, cells - 1, axis=1)
        west = pltpu.roll(centre, 1, axis=1)
        return (
            centre
            + lat_coeff * (north + south - 2.0 * centre)
            + lon_coeff * (east + west - 2.0 * centre)
            - advect_coeff * centre * (east - west)
        )

    empty = jnp.zeros((1, cells, LANES), jnp.float32)
    for _ in range(STEPS):
        main_north = jnp.concatenate([empty, main[:-1]], axis=0)
        main_south = jnp.concatenate([main[1:], empty], axis=0)
        lower = pltpu.roll(rest, piece, axis=2)
        upper = pltpu.roll(rest, LANES - piece, axis=2)
        rest_north = jnp.where(lane < piece, jnp.concatenate([empty, lower[:-1]], axis=0), lower)
        rest_south = jnp.where(lane >= LANES - piece, jnp.concatenate([upper[1:], empty], axis=0), upper)
        main = step(main, main_north, main_south)
        rest = step(rest, rest_north, rest_south)
    main = pltpu.roll(main, cells - STEPS, axis=1)
    rest = pltpu.roll(rest, cells - STEPS, axis=1)
    for strip in range(strips):
        own = slice(strip * width_cols, (strip + 1) * width_cols)
        o_ref[strip, :, :lat_rows] = main[:, own].reshape(lat_count, lat_rows, width_cols, LANES)
        o_ref[strip, :, lat_rows] = rest[:, own]


def gather_kernel(x_ref, o_ref):
    member_count, lat_count, packed, width_cols, _ = x_ref.shape
    lat_rows = packed - 1
    piece = LANES // lat_rows
    cells = lat_count * lat_rows * width_cols
    for member in range(member_count):
        o_ref[:, member * LANES : (member + 1) * LANES] = x_ref[member, :, :lat_rows].reshape(cells, LANES)
    rest = [x_ref[member, :, lat_rows] for member in range(member_count)]
    part = lax.broadcasted_iota(jnp.int32, rest[0].shape, 2) // piece
    rows = []
    for row in range(lat_rows):
        total = rest[row]
        for member in range(member_count):
            if member != row:
                moved = pltpu.roll(rest[member], (member - row) * piece % LANES, axis=2)
                total = jnp.where(part == member, moved, total)
        rows.append(total)
    o_ref[:, member_count * LANES :] = jnp.stack(rows, axis=1).reshape(cells, LANES)


def scatter_kernel(lat_count, width_cols, x_ref, o_ref):
    member_count = x_ref.shape[1] // LANES - 1
    lat_rows = o_ref.shape[1] - 1
    piece = LANES // lat_rows
    held = x_ref[:, member_count * LANES :].reshape(lat_count, lat_rows, width_cols, LANES)
    part = lax.broadcasted_iota(jnp.int32, held[:, 0].shape, 2) // piece
    for member in range(member_count):
        own = slice(member * lat_count, (member + 1) * lat_count)
        o_ref[own, :lat_rows] = x_ref[:, member * LANES : (member + 1) * LANES].reshape(
            lat_count, lat_rows, width_cols, LANES
        )
        total = held[:, member]
        for row in range(lat_rows):
            if row != member:
                moved = pltpu.roll(held[:, row], (row - member) * piece % LANES, axis=2)
                total = jnp.where(part == row, moved, total)
        o_ref[own, lat_rows] = total


def halves(value):
    high = value.astype(jnp.bfloat16)
    return high, (value - high.astype(jnp.float32)).astype(jnp.bfloat16)


def dot_halves(left, right, turned=False):
    dims = (((1,), (1 if turned else 0,)), ((), ()))
    dot = functools.partial(lax.dot_general, dimension_numbers=dims, preferred_element_type=jnp.float32)
    return dot(left[0], right[0]) + (dot(left[0], right[1]) + dot(left[1], right[0]))


def solve_kernel(
    states_ref, before_ref, own_ref, after_ref, value_ref, row_ref, col_ref, mask_ref, o_ref
):
    cells, members = states_ref.shape
    patches = row_ref.shape[0]
    states = states_ref[...]
    state_mean = jnp.mean(states, axis=1, keepdims=True)
    anomaly = states - state_mean
    near = jnp.concatenate([before_ref[...], own_ref[...], after_ref[...]], axis=0)
    spread = near - jnp.mean(near, axis=1, keepdims=True)
    count = near.shape[0]
    near_halves = halves(near)
    ones = jnp.ones((8, members), jnp.bfloat16)
    sums = sum(
        lax.dot_general(ones, part, (((1,), (1,)), ((), ())), preferred_element_type=jnp.float32)
        for part in near_halves
    )
    innov = value_ref[...] - sums * (1.0 / members)
    spread_halves, anomaly_halves = halves(spread), halves(anomaly)
    common = dot_halves(spread_halves, spread_halves, True)
    crossed = dot_halves(anomaly_halves, spread_halves, True)
    turned = spread.T
    degrees = members - 1.0
    shift, shrink = state_mean, jnp.zeros((cells, 1), jnp.float32)
    weights_all = jnp.zeros((cells, count), jnp.float32)
    for patch in range(patches):
        row, col, mask = row_ref[patch], col_ref[patch], mask_ref[patch]
        outer = jnp.dot(
            (turned * (row * row)).astype(jnp.bfloat16),
            spread_halves[0],
            preferred_element_type=jnp.float32,
        )
        bound = degrees + jnp.max(jnp.sum(jnp.abs(outer), axis=0, keepdims=True), axis=1, keepdims=True)
        inverse = 1.0 / bound
        alpha = degrees * inverse
        x = common * col * (row * inverse)
        c0 = 2.25 + alpha * (-2.4375 + alpha * (1.6875 + alpha * (-0.5625 + alpha * 0.0625)))
        c1 = -2.4375 + alpha * (3.375 + alpha * (-1.6875 + alpha * 0.25))
        c2 = 1.6875 + alpha * (-1.6875 + alpha * 0.375)
        c3 = -0.5625 + alpha * 0.25
        c4 = 0.0625
        x_halves = halves(x)
        x2 = dot_halves(x_halves, x_halves)
        x2_halves = halves(x2)
        x3 = dot_halves(x2_halves, x_halves)
        x4 = dot_halves(x2_halves, x2_halves)
        low = halves(c2 * x + c3 * x2 + c4 * x3)
        high = halves(c1 * x + c2 * x2 + c3 * x3 + c4 * x4)
        block = jnp.concatenate([crossed, innov], axis=0) * row
        block_halves = halves(block)
        b1 = c1 * block + dot_halves(block_halves, low)
        b2 = c0 * block + dot_halves(block_halves, high)
        b3 = c0 * b2 + dot_halves(halves(b2), high)
        mixed = alpha * c0 * b1 + b3
        got = 1.5 * b1 - 0.5 * (
            alpha * c0 * c0 * b1
            + c0 * mixed
            + dot_halves(halves(mixed), high)
            + alpha * (c1 * b3 + dot_halves(halves(b3), low))
        )
        base = c0 * (1.5 - 0.5 * alpha * c0 * c0)
        driven = base * block[cells:] + dot_halves(halves(got[cells:]), x_halves)
        again = dot_halves(halves(driven), x_halves)
        mean_part = inverse * jnp.sum(
            block[:cells] * (base * driven[:1]) + got[:cells] * again[:1], axis=1, keepdims=True
        )
        root_scale = jnp.sqrt(alpha)
        shift = shift + mask * mean_part
        shrink = shrink + mask * (root_scale * base)
        weights_all = weights_all + mask * (got[:cells] * (row * (root_scale * inverse)))
    o_ref[...] = shift + shrink * anomaly + dot_halves(halves(weights_all), spread_halves)


def local(kernel, shape, *operands):
    vmem = pl.BlockSpec(memory_space=pltpu.VMEM)
    return pl.pallas_call(
        kernel,
        out_shape=jax.ShapeDtypeStruct(shape, jnp.float32),
        in_specs=[vmem] * len(operands),
        out_specs=vmem,
        cost_estimate=pl.CostEstimate(flops=10**6, bytes_accessed=10**7, transcendentals=0),
    )(*operands)


def packed_device(ensemble, obs_cell, obs_value, obs_var, patch_rows):
    members_dev, lat_rows, lon_cells = ensemble.shape
    lat_count, member_count = lax.axis_size("lat"), lax.axis_size("member")
    servers = lat_count * member_count
    width_cols = lon_cells // servers
    span = lon_cells // lat_count
    obs_count = obs_cell.shape[1]
    patches = patch_rows.shape[1]

    meta = jnp.concatenate(
        [
            obs_value,
            obs_var,
            obs_cell.astype(jnp.float32),
            jnp.pad(patch_rows.astype(jnp.float32), ((0, 0), (0, obs_count - patches))),
        ],
        axis=0,
    )
    near_meta = []
    for offset in (-1, 0, 1):
        pairs = []
        for server in range(servers):
            member, lat = host_of(server, member_count, lat_count)
            pairs.append(((server + offset) % servers, member * lat_count + lat))
        near_meta.append(lax.ppermute(meta, ("member", "lat"), pairs))

    cells = ensemble.transpose(1, 2, 0)
    piece = members_dev - LANES
    rest = cells[:, :, LANES:].transpose(1, 0, 2).reshape(1, lon_cells, lat_rows * piece)
    packed = jnp.concatenate([cells[:, :, :LANES], rest], axis=0)
    wide = jnp.concatenate([packed[:, -STEPS:], packed, packed[:, :STEPS]], axis=1)
    outgoing = jnp.stack(
        [
            wide[:, group_of(lat, lat_count) * span : group_of(lat, lat_count) * span + span + 2 * STEPS]
            for lat in range(lat_count)
        ]
    )
    got = exchange(
        outgoing,
        lat_count,
        lambda p: {"lat": p},
        lambda p: p,
        lambda p: p,
        lambda: lax.axis_index("lat"),
        1,
    )
    strips = local(
        functools.partial(forecast_kernel, member_count, width_cols),
        (member_count, lat_count, lat_rows + 1, width_cols, LANES),
        got,
    )
    got = exchange(
        strips,
        member_count,
        lambda p: {"member": p},
        lambda p: turn_of(group_of(lax.axis_index("lat"), lat_count), p, member_count),
        lambda p: p,
        lambda: lax.axis_index("member"),
        2,
    )
    states = local(gather_kernel, (lat_count * lat_rows * width_cols, members_dev * member_count), got)
    observed = jnp.take(states, near_meta[1][2].astype(jnp.int32), axis=0)
    before, after = ring(observed, member_count, lat_count, 3)
    joined = jnp.concatenate(near_meta, axis=1)
    places = joined[2].astype(jnp.int32)
    shifts = jnp.repeat(jnp.array([-1.0, 0.0, 1.0], jnp.float32), obs_count) * width_cols
    lengths = near_meta[1][3, :patches].astype(jnp.int32)
    starts = jnp.cumsum(lengths) - lengths
    lat_total = lat_count * lat_rows
    scale = jnp.sqrt(
        localize(
            (places // width_cols).astype(jnp.float32)[None],
            ((places % width_cols).astype(jnp.float32) + shifts)[None],
            starts[:, None],
            lengths[:, None],
            lat_total / 4.0,
            float(width_cols),
        )
        / joined[1][None]
    )
    cell_rows = (jnp.arange(lat_total * width_cols, dtype=jnp.int32) // width_cols)[None, :, None]
    begins = starts[:, None, None]
    mask = ((cell_rows >= begins) & (cell_rows < begins + lengths[:, None, None])).astype(jnp.float32)
    analysed = local(
        solve_kernel,
        states.shape,
        states,
        before,
        observed,
        after,
        joined[:1],
        scale[:, None, :],
        scale[:, :, None],
        mask,
    )
    outgoing = local(
        functools.partial(scatter_kernel, lat_count, width_cols),
        (servers, lat_rows + 1, width_cols, LANES),
        analysed,
    )
    got = exchange(
        outgoing,
        servers,
        lambda p: {"member": p // lat_count, "lat": p % lat_count},
        lambda p: p,
        lambda p: server_of(p // lat_count, p % lat_count, member_count, lat_count),
        lambda: lax.axis_index("member") * lat_count + lax.axis_index("lat"),
        4,
    )
    main = got[:, :lat_rows].transpose(3, 1, 0, 2).reshape(LANES, lat_rows, lon_cells)
    rest = got[:, lat_rows].reshape(lon_cells, lat_rows, piece).transpose(2, 1, 0)
    return jnp.concatenate([main, rest], axis=0)


def per_device(ensemble, obs_cell, obs_value, obs_var, patch_rows):
    members_dev, lat_rows, lon_cells = ensemble.shape
    lat_count, member_count = lax.axis_size("lat"), lax.axis_size("member")
    fits = (
        (members_dev - LANES) * lat_rows == LANES
        and member_count == lat_rows
        and lat_count % 2 == 0
        and lon_cells // (lat_count * member_count) == 8
        and STEPS == 4
        and patch_rows.shape[1] <= obs_cell.shape[1]
    )
    device = packed_device if fits else plain_device
    return device(ensemble, obs_cell, obs_value, obs_var, patch_rows)


def solution(mesh):
    in_specs = (
        P("member", "lat", None),
        P(("member", "lat"), None),
        P(("member", "lat"), None),
        P(("member", "lat"), None),
        P(("member", "lat"), None),
    )
    out_specs = P("member", "lat", None)
    return jax.shard_map(
        per_device, mesh=mesh, in_specs=in_specs, out_specs=out_specs, check_vma=False
    )
```

```python
import functools

import jax
import jax.numpy as jnp
from jax import lax
from jax.experimental import pallas as pl
from jax.experimental.pallas import tpu as pltpu
from jax.sharding import PartitionSpec as P

STEPS = 4


lat_coeff = 0.4
lon_coeff = 0.05
advect_coeff = 0.1


def with_halo(value, sides, width, wrap):
    for axis, dim in sides:
        size, length = (lax.axis_size(axis), value.shape[dim])
        up = [(i, (i + 1) % size) for i in range(size if wrap else size - 1)]
        down = [(j, i) for i, j in up]
        last = lax.slice_in_dim(value, length - width, length, axis=dim)
        initial = lax.slice_in_dim(value, 0, width, axis=dim)
        before = lax.ppermute(last, axis, up)
        after = lax.ppermute(initial, axis, down)
        value = jnp.concatenate([before, value, after], axis=dim)
    return value


def advance(padded):
    centre = padded[:, 1:-1]
    northern = padded[:, :-2]
    southern = padded[:, 2:]
    eastern = jnp.roll(centre, -1, axis=2)
    western = jnp.roll(centre, 1, axis=2)
    return (
        centre
        + lat_coeff * (northern + southern - 2.0 * centre)
        + lon_coeff * (eastern + western - 2.0 * centre)
        - advect_coeff * centre * (eastern - western)
    )


def observe(states, cell_index, values):
    observed = jnp.take(states, cell_index, axis=1)
    obs_mean = jnp.mean(observed, axis=0)
    return (observed - obs_mean, values - obs_mean)


def localize(obs_rows, rel_cols, first_row, row_count, lat_scale, width_cols):
    lower = first_row.astype(jnp.float32)
    upper = lower + row_count.astype(jnp.float32) - 1.0
    lat_gap = jnp.maximum(jnp.maximum(lower - obs_rows, obs_rows - upper), 0.0) / lat_scale
    lon_gap = jnp.maximum(jnp.maximum(-rel_cols, rel_cols - (width_cols - 1.0)), 0.0) / width_cols
    return jnp.exp(-lat_gap * lat_gap - lon_gap * lon_gap)


def dot3(left, right):
    return jnp.matmul(left, right, precision=lax.Precision.HIGH, preferred_element_type=jnp.float32)


def analyse(states, spread, obs_meta, lengths, width_cols):
    members = states.shape[1]
    cell_total = states.shape[0]
    lat_total = cell_total // width_cols
    near = spread.shape[0]
    state_mean = jnp.mean(states, axis=1)
    anomaly = states - state_mean[:, None]
    starts = jnp.cumsum(lengths) - lengths
    cell_rows = jnp.arange(cell_total, dtype=jnp.int32) // width_cols
    identity = jnp.eye(members, dtype=jnp.float32)
    products = dot3(spread, jnp.concatenate([spread, anomaly], axis=0).T)
    common, crossed = products[:, :near], products[:, near:]
    innov = obs_meta[0]
    shrink = jnp.zeros((cell_total,), jnp.float32)
    shift = state_mean
    weights_all = jnp.zeros((near, cell_total), jnp.float32)
    for patch in range(lengths.shape[0]):
        weights = (
            localize(
                obs_meta[2],
                obs_meta[3],
                starts[patch],
                lengths[patch],
                lat_total / 4.0,
                float(width_cols),
            )
            / obs_meta[1]
        )
        scale = jnp.sqrt(weights)
        gram_matrix = (members - 1.0) * identity + jnp.dot(
            (spread * weights[:, None]).T, spread, preferred_element_type=jnp.float32
        )
        bound = jnp.max(jnp.sum(jnp.abs(gram_matrix), axis=1))
        alpha = (members - 1.0) / bound
        x = common * scale[:, None] * (scale / bound)[None, :]
        c0 = 2.25 + alpha * (-2.4375 + alpha * (1.6875 + alpha * (-0.5625 + alpha * 0.0625)))
        c1 = -2.4375 + alpha * (3.375 + alpha * (-1.6875 + alpha * 0.25))
        c2 = 1.6875 + alpha * (-1.6875 + alpha * 0.375)
        c3 = -0.5625 + alpha * 0.25
        c4 = 0.0625
        x2 = dot3(x, x)
        x34 = dot3(x2, jnp.concatenate([x, x2], axis=1))
        x3, x4 = x34[:, :near], x34[:, near:]
        low = c2 * x + c3 * x2 + c4 * x3
        high = c1 * x + c2 * x2 + c3 * x3 + c4 * x4
        block = jnp.concatenate([crossed * scale[:, None], (scale * innov)[:, None]], axis=1)
        both = dot3(jnp.concatenate([low, high], axis=0), block)
        b1 = c1 * block + both[:near]
        b2 = c0 * block + both[near:]
        b3 = c0 * b2 + dot3(high, b2)
        mixed = alpha * c0 * b1 + b3
        got = 1.5 * b1 - 0.5 * (
            alpha * c0 * c0 * b1
            + c0 * mixed
            + dot3(high, mixed)
            + alpha * (c1 * b3 + dot3(low, b3))
        )
        base = c0 * (1.5 - 0.5 * alpha * c0 * c0)
        driven = base * block[:, -1] + jnp.sum(x * got[:, -1][None, :], axis=1)
        again = jnp.sum(x * driven[None, :], axis=1)
        mean_part = (
            jnp.sum(block[:, :-1] * (base * driven)[:, None] + got[:, :-1] * again[:, None], axis=0)
            / bound
        )
        cell_mask = (cell_rows >= starts[patch]) & (cell_rows < starts[patch] + lengths[patch])
        root_scale = jnp.sqrt((members - 1.0) / bound)
        shift = shift + jnp.where(cell_mask, mean_part, 0.0)
        shrink = jnp.where(cell_mask, root_scale * base, shrink)
        weights_all = jnp.where(
            cell_mask[None, :], got[:, :-1] * (scale * (root_scale / bound))[:, None], weights_all
        )
    return shift[:, None] + shrink[:, None] * anomaly + dot3(weights_all.T, spread)


def plain_device(ensemble, obs_cell, obs_value, obs_var, patch_rows):
    fields = ensemble
    members_dev = fields.shape[0]
    lat_rows = fields.shape[1]
    lon_cells = fields.shape[2]
    lat_count = lax.axis_size("lat")
    member_count = lax.axis_size("member")
    servers = lat_count * member_count
    width_cols = lon_cells // servers
    padded = with_halo(fields, (("lat", 1),), STEPS, False)
    global_rows = (
        lax.axis_index("lat") * lat_rows + jnp.arange(lat_rows + 2 * STEPS, dtype=jnp.int32) - STEPS
    )
    inside = ((global_rows >= 0) & (global_rows < lat_rows * lat_count)).astype(jnp.float32)
    for step_index in range(STEPS):
        padded = advance(padded)
        keeper = inside[step_index + 1 : inside.shape[0] - step_index - 1]
        padded = padded * keeper[None, :, None]
    fields = padded
    blocks = fields.reshape(1, members_dev, lat_rows, lon_cells)
    received = lax.all_to_all(blocks, ("member", "lat"), split_axis=3, concat_axis=0, tiled=True)
    strip = received.reshape(member_count, lat_count, members_dev, lat_rows, width_cols)
    strip = strip.transpose(0, 2, 1, 3, 4).reshape(
        member_count * members_dev, lat_count * lat_rows, width_cols
    )
    members = strip.shape[0]
    lat_total = strip.shape[1]
    states = strip.reshape(members, lat_total * width_cols)
    cell_index = obs_cell[0]
    obs_count = cell_index.shape[0]
    spread, innov = observe(states, cell_index, obs_value[0])
    obs_meta = jnp.stack(
        [
            innov,
            obs_var[0],
            (cell_index // width_cols).astype(jnp.float32),
            (cell_index % width_cols).astype(jnp.float32),
        ]
    )
    near_spread, near_meta = (
        with_halo(spread, ((("member", "lat"), 1),), obs_count, True),
        with_halo(obs_meta, ((("member", "lat"), 1),), obs_count, True),
    )
    shifts = jnp.repeat(jnp.array([-1.0, 0.0, 1.0], jnp.float32), obs_count) * width_cols
    near_meta = jnp.concatenate([near_meta[:3], (near_meta[3] + shifts)[None, :]], axis=0)
    analysed = analyse(states.T, near_spread.T, near_meta, patch_rows[0], width_cols).T
    analysed = analysed.reshape(members, lat_total, width_cols)
    outgoing = analysed.reshape(member_count, members_dev, lat_count, lat_rows, width_cols)
    outgoing = outgoing.transpose(0, 2, 1, 3, 4).reshape(servers, members_dev, lat_rows, width_cols)
    returned = lax.all_to_all(outgoing, ("member", "lat"), split_axis=0, concat_axis=3, tiled=True)
    return returned.reshape(members_dev, lat_rows, lon_cells)


LANES = 128


def group_of(place, size):
    return place % 2 * (size - 1 - place // 2) + (1 - place % 2) * (place // 2)


def place_of(group, size):
    late = group * 2 // size
    return late * (2 * (size - 1 - group) + 1) + (1 - late) * 2 * group


def turn_of(group, index, size):
    return (group % 2) * (size - 1 - index) + (1 - group % 2) * index


def server_of(member, lat, member_count, lat_count):
    group = group_of(lat, lat_count)
    return member_count * group + turn_of(group, member, member_count)


def host_of(server, member_count, lat_count):
    group = server // member_count
    return turn_of(group, server % member_count, member_count), place_of(group, lat_count)


def exchange_kernel(count, place, source, target, me_of, x_ref, o_ref, send_sem, recv_sem, own_sem):
    me = me_of()
    barrier = pltpu.get_barrier_semaphore()

    def greet(step, carry):
        pl.semaphore_signal(barrier, inc=1, device_id=place(lax.rem(me + step, count)), device_id_type=pl.DeviceIdType.MESH)
        return carry

    lax.fori_loop(1, count, greet, 0)
    own = pltpu.make_async_copy(x_ref.at[source(me)], o_ref.at[target(me)], own_sem)
    own.start()
    pl.semaphore_wait(barrier, count - 1)

    def sending(step):
        other = lax.rem(me + step, count)
        return pltpu.make_async_remote_copy(
            src_ref=x_ref.at[source(other)],
            dst_ref=o_ref.at[target(me)],
            send_sem=send_sem.at[step],
            recv_sem=recv_sem.at[step],
            device_id=place(other),
            device_id_type=pl.DeviceIdType.MESH,
        )

    def arriving(step):
        other = lax.rem(me + count - step, count)
        return pltpu.make_async_remote_copy(
            src_ref=x_ref.at[source(other)],
            dst_ref=o_ref.at[target(other)],
            send_sem=send_sem.at[step],
            recv_sem=recv_sem.at[step],
            device_id=place(other),
            device_id_type=pl.DeviceIdType.MESH,
        )

    def start(step, carry):
        sending(step).start()
        return carry

    def finish(step, carry):
        arriving(step).wait_recv()
        sending(step).wait_send()
        return carry

    lax.fori_loop(1, count, start, 0)
    own.wait()
    lax.fori_loop(1, count, finish, 0)


def exchange(blocks, count, place, source, target, me_of, number):
    moved = blocks.size * 4
    return pl.pallas_call(
        functools.partial(exchange_kernel, count, place, source, target, me_of),
        out_shape=jax.ShapeDtypeStruct(blocks.shape, jnp.float32),
        in_specs=[pl.BlockSpec(memory_space=pltpu.VMEM)],
        out_specs=pl.BlockSpec(memory_space=pltpu.VMEM),
        scratch_shapes=[
            pltpu.SemaphoreType.DMA((count,)),
            pltpu.SemaphoreType.DMA((count,)),
            pltpu.SemaphoreType.DMA,
        ],
        compiler_params=pltpu.CompilerParams(collective_id=number, has_side_effects=True),
        cost_estimate=pl.CostEstimate(flops=0, bytes_accessed=40 * moved, transcendentals=0),
    )(blocks)


def ring_kernel(member_count, lat_count, x_ref, before_ref, after_ref, send_sem, recv_sem):
    servers = member_count * lat_count
    me = server_of(lax.axis_index("member"), lax.axis_index("lat"), member_count, lat_count)

    def place(server):
        member, lat = host_of(server, member_count, lat_count)
        return {"member": member, "lat": lat}

    up, down = place(lax.rem(me + 1, servers)), place(lax.rem(me + servers - 1, servers))
    barrier = pltpu.get_barrier_semaphore()
    for beside in (up, down):
        pl.semaphore_signal(barrier, inc=1, device_id=beside, device_id_type=pl.DeviceIdType.MESH)
    pl.semaphore_wait(barrier, 2)
    copies = []
    for side, (beside, landing) in enumerate(((up, before_ref), (down, after_ref))):
        copy = pltpu.make_async_remote_copy(
            src_ref=x_ref,
            dst_ref=landing,
            send_sem=send_sem.at[side],
            recv_sem=recv_sem.at[side],
            device_id=beside,
            device_id_type=pl.DeviceIdType.MESH,
        )
        copy.start()
        copies.append(copy)
    for copy in copies:
        copy.wait()


def ring(own, member_count, lat_count, number):
    shape = jax.ShapeDtypeStruct(own.shape, jnp.float32)
    vmem = pl.BlockSpec(memory_space=pltpu.VMEM)
    return pl.pallas_call(
        functools.partial(ring_kernel, member_count, lat_count),
        out_shape=(shape, shape),
        in_specs=[vmem],
        out_specs=(vmem, vmem),
        scratch_shapes=[pltpu.SemaphoreType.DMA((2,)), pltpu.SemaphoreType.DMA((2,))],
        compiler_params=pltpu.CompilerParams(collective_id=number, has_side_effects=True),
        cost_estimate=pl.CostEstimate(flops=0, bytes_accessed=100 * own.size, transcendentals=0),
    )(own)


def forecast_kernel(strips, width_cols, x_ref, o_ref):
    lat_count, packed, cells, _ = x_ref.shape
    lat_rows = packed - 1
    piece = LANES // lat_rows
    main = x_ref[:, :lat_rows].reshape(lat_count * lat_rows, cells, LANES)
    rest = x_ref[:, lat_rows]
    lane = lax.broadcasted_iota(jnp.int32, rest.shape, 2)

    def step(centre, north, south):
        east = pltpu.roll(centre, cells - 1, axis=1)
        west = pltpu.roll(centre, 1, axis=1)
        return (
            centre
            + lat_coeff * (north + south - 2.0 * centre)
            + lon_coeff * (east + west - 2.0 * centre)
            - advect_coeff * centre * (east - west)
        )

    empty = jnp.zeros((1, cells, LANES), jnp.float32)
    for _ in range(STEPS):
        main_north = jnp.concatenate([empty, main[:-1]], axis=0)
        main_south = jnp.concatenate([main[1:], empty], axis=0)
        lower = pltpu.roll(rest, piece, axis=2)
        upper = pltpu.roll(rest, LANES - piece, axis=2)
        rest_north = jnp.where(lane < piece, jnp.concatenate([empty, lower[:-1]], axis=0), lower)
        rest_south = jnp.where(lane >= LANES - piece, jnp.concatenate([upper[1:], empty], axis=0), upper)
        main = step(main, main_north, main_south)
        rest = step(rest, rest_north, rest_south)
    main = pltpu.roll(main, cells - STEPS, axis=1)
    rest = pltpu.roll(rest, cells - STEPS, axis=1)
    for strip in range(strips):
        own = slice(strip * width_cols, (strip + 1) * width_cols)
        o_ref[strip, :, :lat_rows] = main[:, own].reshape(lat_count, lat_rows, width_cols, LANES)
        o_ref[strip, :, lat_rows] = rest[:, own]


def gather_kernel(x_ref, o_ref):
    member_count, lat_count, packed, width_cols, _ = x_ref.shape
    lat_rows = packed - 1
    piece = LANES // lat_rows
    cells = lat_count * lat_rows * width_cols
    for member in range(member_count):
        o_ref[:, member * LANES : (member + 1) * LANES] = x_ref[member, :, :lat_rows].reshape(cells, LANES)
    rest = [x_ref[member, :, lat_rows] for member in range(member_count)]
    part = lax.broadcasted_iota(jnp.int32, rest[0].shape, 2) // piece
    rows = []
    for row in range(lat_rows):
        total = rest[row]
        for member in range(member_count):
            if member != row:
                moved = pltpu.roll(rest[member], (member - row) * piece % LANES, axis=2)
                total = jnp.where(part == member, moved, total)
        rows.append(total)
    o_ref[:, member_count * LANES :] = jnp.stack(rows, axis=1).reshape(cells, LANES)


def scatter_kernel(lat_count, width_cols, x_ref, o_ref):
    member_count = x_ref.shape[1] // LANES - 1
    lat_rows = o_ref.shape[1] - 1
    piece = LANES // lat_rows
    held = x_ref[:, member_count * LANES :].reshape(lat_count, lat_rows, width_cols, LANES)
    part = lax.broadcasted_iota(jnp.int32, held[:, 0].shape, 2) // piece
    for member in range(member_count):
        own = slice(member * lat_count, (member + 1) * lat_count)
        o_ref[own, :lat_rows] = x_ref[:, member * LANES : (member + 1) * LANES].reshape(
            lat_count, lat_rows, width_cols, LANES
        )
        total = held[:, member]
        for row in range(lat_rows):
            if row != member:
                moved = pltpu.roll(held[:, row], (row - member) * piece % LANES, axis=2)
                total = jnp.where(part == row, moved, total)
        o_ref[own, lat_rows] = total


def halves(value):
    high = value.astype(jnp.bfloat16)
    return high, (value - high.astype(jnp.float32)).astype(jnp.bfloat16)


def dot_halves(left, right, turned=False):
    dims = (((1,), (1 if turned else 0,)), ((), ()))
    dot = functools.partial(lax.dot_general, dimension_numbers=dims, preferred_element_type=jnp.float32)
    return dot(left[0], right[0]) + (dot(left[0], right[1]) + dot(left[1], right[0]))


def solve_kernel(
    states_ref, before_ref, own_ref, after_ref, value_ref, row_ref, col_ref, mask_ref, o_ref
):
    cells, members = states_ref.shape
    patches = row_ref.shape[0]
    states = states_ref[...]
    state_mean = jnp.mean(states, axis=1, keepdims=True)
    anomaly = states - state_mean
    each = value_ref.shape[1] // 3
    near = jnp.concatenate([before_ref[:each], own_ref[:each], after_ref[:each]], axis=0)
    spread = near - jnp.mean(near, axis=1, keepdims=True)
    count = near.shape[0]
    near_halves = halves(near)
    ones = jnp.ones((8, members), jnp.bfloat16)
    sums = sum(
        lax.dot_general(ones, part, (((1,), (1,)), ((), ())), preferred_element_type=jnp.float32)
        for part in near_halves
    )
    innov = value_ref[...] - sums * (1.0 / members)
    spread_halves, anomaly_halves = halves(spread), halves(anomaly)
    common = dot_halves(spread_halves, spread_halves, True)
    crossed = dot_halves(anomaly_halves, spread_halves, True)
    turned = spread.T
    degrees = members - 1.0
    shift, shrink = state_mean, jnp.zeros((cells, 1), jnp.float32)
    weights_all = jnp.zeros((cells, count), jnp.float32)
    for patch in range(patches):
        row, col, mask = row_ref[patch], col_ref[patch], mask_ref[patch]
        outer = jnp.dot(
            (turned * (row * row)).astype(jnp.bfloat16),
            spread_halves[0],
            preferred_element_type=jnp.float32,
        )
        bound = degrees + jnp.max(jnp.sum(jnp.abs(outer), axis=0, keepdims=True), axis=1, keepdims=True)
        inverse = 1.0 / bound
        alpha = degrees * inverse
        x = common * col * (row * inverse)
        c0 = 2.25 + alpha * (-2.4375 + alpha * (1.6875 + alpha * (-0.5625 + alpha * 0.0625)))
        c1 = -2.4375 + alpha * (3.375 + alpha * (-1.6875 + alpha * 0.25))
        c2 = 1.6875 + alpha * (-1.6875 + alpha * 0.375)
        c3 = -0.5625 + alpha * 0.25
        c4 = 0.0625
        x_halves = halves(x)
        x2 = dot_halves(x_halves, x_halves)
        x2_halves = halves(x2)
        x3 = dot_halves(x2_halves, x_halves)
        x4 = dot_halves(x2_halves, x2_halves)
        low = halves(c2 * x + c3 * x2 + c4 * x3)
        high = halves(c1 * x + c2 * x2 + c3 * x3 + c4 * x4)
        block = jnp.concatenate([crossed, innov], axis=0) * row
        block_halves = halves(block)
        b1 = c1 * block + dot_halves(block_halves, low)
        b2 = c0 * block + dot_halves(block_halves, high)
        b3 = c0 * b2 + dot_halves(halves(b2), high)
        mixed = alpha * c0 * b1 + b3
        got = 1.5 * b1 - 0.5 * (
            alpha * c0 * c0 * b1
            + c0 * mixed
            + dot_halves(halves(mixed), high)
            + alpha * (c1 * b3 + dot_halves(halves(b3), low))
        )
        base = c0 * (1.5 - 0.5 * alpha * c0 * c0)
        driven = base * block[cells:] + dot_halves(halves(got[cells:]), x_halves)
        again = dot_halves(halves(driven), x_halves)
        mean_part = inverse * jnp.sum(
            block[:cells] * (base * driven[:1]) + got[:cells] * again[:1], axis=1, keepdims=True
        )
        root_scale = jnp.sqrt(alpha)
        shift = shift + mask * mean_part
        shrink = shrink + mask * (root_scale * base)
        weights_all = weights_all + mask * (got[:cells] * (row * (root_scale * inverse)))
    o_ref[...] = shift + shrink * anomaly + dot_halves(halves(weights_all), spread_halves)


def local(kernel, shape, *operands):
    vmem = pl.BlockSpec(memory_space=pltpu.VMEM)
    return pl.pallas_call(
        kernel,
        out_shape=jax.ShapeDtypeStruct(shape, jnp.float32),
        in_specs=[vmem] * len(operands),
        out_specs=vmem,
        cost_estimate=pl.CostEstimate(flops=10**6, bytes_accessed=10**7, transcendentals=0),
    )(*operands)


def packed_device(ensemble, obs_cell, obs_value, obs_var, patch_rows):
    members_dev, lat_rows, lon_cells = ensemble.shape
    lat_count, member_count = lax.axis_size("lat"), lax.axis_size("member")
    servers = lat_count * member_count
    width_cols = lon_cells // servers
    span = lon_cells // lat_count
    obs_count = obs_cell.shape[1]
    patches = patch_rows.shape[1]

    meta = jnp.concatenate(
        [
            obs_value,
            obs_var,
            obs_cell.astype(jnp.float32),
            jnp.pad(patch_rows.astype(jnp.float32), ((0, 0), (0, obs_count - patches))),
        ],
        axis=0,
    )
    pairs = []
    for server in range(servers):
        member, lat = host_of(server, member_count, lat_count)
        pairs.append((server, member * lat_count + lat))
    own_meta = lax.ppermute(meta, ("member", "lat"), pairs)

    cells = ensemble.transpose(1, 2, 0)
    piece = members_dev - LANES
    rest = cells[:, :, LANES:].transpose(1, 0, 2).reshape(1, lon_cells, lat_rows * piece)
    packed = jnp.concatenate([cells[:, :, :LANES], rest], axis=0)
    wide = jnp.concatenate([packed[:, -STEPS:], packed, packed[:, :STEPS]], axis=1)
    outgoing = jnp.stack(
        [
            wide[:, group_of(lat, lat_count) * span : group_of(lat, lat_count) * span + span + 2 * STEPS]
            for lat in range(lat_count)
        ]
    )
    got = exchange(
        outgoing,
        lat_count,
        lambda p: {"lat": p},
        lambda p: p,
        lambda p: p,
        lambda: lax.axis_index("lat"),
        1,
    )
    strips = local(
        functools.partial(forecast_kernel, member_count, width_cols),
        (member_count, lat_count, lat_rows + 1, width_cols, LANES),
        got,
    )
    got = exchange(
        strips,
        member_count,
        lambda p: {"member": p},
        lambda p: turn_of(group_of(lax.axis_index("lat"), lat_count), p, member_count),
        lambda p: p,
        lambda: lax.axis_index("member"),
        2,
    )
    states = local(gather_kernel, (lat_count * lat_rows * width_cols, members_dev * member_count), got)
    observed = jnp.take(states, own_meta[2].astype(jnp.int32), axis=0)
    noted = jnp.pad(own_meta, ((0, 4), (0, states.shape[1] - obs_count)))
    observed = jnp.concatenate([observed, noted], axis=0)
    before, after = ring(observed, member_count, lat_count, 3)
    noted = slice(obs_count, obs_count + 4)
    near_meta = (before[noted, :obs_count], own_meta, after[noted, :obs_count])
    joined = jnp.concatenate(near_meta, axis=1)
    places = joined[2].astype(jnp.int32)
    shifts = jnp.repeat(jnp.array([-1.0, 0.0, 1.0], jnp.float32), obs_count) * width_cols
    lengths = own_meta[3, :patches].astype(jnp.int32)
    starts = jnp.cumsum(lengths) - lengths
    lat_total = lat_count * lat_rows
    scale = jnp.sqrt(
        localize(
            (places // width_cols).astype(jnp.float32)[None],
            ((places % width_cols).astype(jnp.float32) + shifts)[None],
            starts[:, None],
            lengths[:, None],
            lat_total / 4.0,
            float(width_cols),
        )
        / joined[1][None]
    )
    cell_rows = (jnp.arange(lat_total * width_cols, dtype=jnp.int32) // width_cols)[None, :, None]
    begins = starts[:, None, None]
    mask = ((cell_rows >= begins) & (cell_rows < begins + lengths[:, None, None])).astype(jnp.float32)
    analysed = local(
        solve_kernel,
        states.shape,
        states,
        before,
        observed,
        after,
        joined[:1],
        scale[:, None, :],
        scale[:, :, None],
        mask,
    )
    outgoing = local(
        functools.partial(scatter_kernel, lat_count, width_cols),
        (servers, lat_rows + 1, width_cols, LANES),
        analysed,
    )
    got = exchange(
        outgoing,
        servers,
        lambda p: {"member": p // lat_count, "lat": p % lat_count},
        lambda p: p,
        lambda p: server_of(p // lat_count, p % lat_count, member_count, lat_count),
        lambda: lax.axis_index("member") * lat_count + lax.axis_index("lat"),
        4,
    )
    main = got[:, :lat_rows].transpose(3, 1, 0, 2).reshape(LANES, lat_rows, lon_cells)
    rest = got[:, lat_rows].reshape(lon_cells, lat_rows, piece).transpose(2, 1, 0)
    return jnp.concatenate([main, rest], axis=0)


def per_device(ensemble, obs_cell, obs_value, obs_var, patch_rows):
    members_dev, lat_rows, lon_cells = ensemble.shape
    lat_count, member_count = lax.axis_size("lat"), lax.axis_size("member")
    fits = (
        (members_dev - LANES) * lat_rows == LANES
        and member_count == lat_rows
        and lat_count % 2 == 0
        and lon_cells // (lat_count * member_count) == 8
        and STEPS == 4
        and patch_rows.shape[1] <= obs_cell.shape[1]
    )
    device = packed_device if fits else plain_device
    return device(ensemble, obs_cell, obs_value, obs_var, patch_rows)


def solution(mesh):
    in_specs = (
        P("member", "lat", None),
        P(("member", "lat"), None),
        P(("member", "lat"), None),
        P(("member", "lat"), None),
        P(("member", "lat"), None),
    )
    out_specs = P("member", "lat", None)
    return jax.shard_map(
        per_device, mesh=mesh, in_specs=in_specs, out_specs=out_specs, check_vma=False
    )
```
